32 devices in a mesh: rep: 2 (over x), px: 4 (over y, core), py: 4 (over z).
Axes of the slice: x: 2, y: 2, z: 4, core: 2. Of those that a mesh axis runs over, the one named last changes fastest.
Arguments:
- density: float32 [4, 128, 128, 128], P('rep', 'px', 'py'), parts along dimension 0, may hold values from -6 to 6
- kernel_factors: float32 [3, 89, 256], replicated, as said below
Outputs:
- potential: float32 [4, 128, 128, 128], P('rep', 'px', 'py'), parts along dimension 0
The draws below stay inside these ranges and needn't reach their ends.
There are 2 independent parts, one for each index of `rep`. The reference program is written for one: setup_inputs(seed, part) draws one part's arguments, and reference() takes and returns one part's arrays. A program takes and returns all parts, laid end to end along the dimension named above; an argument that names none is the same for every part. Nothing has to cross between parts.
Inputs may be any that keep to these rules, and one draw needn't show every extreme that they name: Each factor is even in its frequency, kernel_factors[d, g, k] = kernel_factors[d, g, 256 - k], and is zero at k = 128.
All inputs are finite; a program needn't handle non-finite values.
Results may differ from the reference program's by a relative error of at most 0.00005.
Values sent between devices are 32-bit elements; how exact they have to be, the bound alone decides.
A program may use at most 128 MiB of HBM per device.

```python
import math
import jax
import jax.numpy as jnp
from jax import lax

N = 128
G = 89
B = 2
M = 256


def draw_kernel_factors(key, part):
    first_key, second_key = jax.random.split(jax.random.fold_in(key, 7))
    widths = jnp.exp(jax.random.uniform(first_key, (G,), jnp.float32, math.log(0.05), math.log(50.0)))
    weights = 20.0 / G * jnp.exp(jax.random.uniform(second_key, (G,), jnp.float32, math.log(0.5), math.log(2.0)))
    frequency = jnp.arange(M, dtype=jnp.int32)
    wrapped = jnp.minimum(frequency, M - frequency).astype(jnp.float32)
    argument = (2.0 * math.pi * wrapped / M) ** 2
    inside = (wrapped < N).astype(jnp.float32)
    base = jnp.exp(-widths[:, None] * argument[None, :]) * inside[None, :]
    return jnp.stack([base * weights[:, None], base, base], 0).astype(jnp.float32)


def levels(stream_key, extent, cuts, smallest, high):
    gain, own = 1.0, jax.random.fold_in(stream_key, 6)
    for dim, blocks in cuts:
        draws = jnp.exp(jax.random.uniform(jax.random.fold_in(own, dim), (blocks,), jnp.float32, smallest / len(cuts), high / len(cuts)))
        gain = gain * jnp.repeat(draws, extent[dim] // blocks).reshape([-1 if axis == dim else 1 for axis in range(len(extent))])
    return gain


def centred(key, shape, spread, most, pieces=(), held_as=jnp.bfloat16):
    level = levels(key, shape, pieces, -0.22, 0.18) if pieces else 1.0
    entries = jax.random.normal(key, shape, jnp.float32) * spread * level
    return jnp.minimum(jnp.maximum(entries, -most), most).astype(held_as)


def setup_inputs(seed: int = 0, part: int = 0) -> dict:
    key_of = jax.random.split(jax.random.key(seed), 3)
    part_splits = jax.random.split(jax.random.fold_in(key_of[2], part), 3)
    return {
        "density": centred(part_splits[0], (B, N, N, N), 1.0, 6.0, ((1, 4), (2, 4)), jnp.float32),
        "kernel_factors": draw_kernel_factors(jax.random.fold_in(key_of[2], 71), part),
    }


def reference(density, kernel_factors):
    highest = lax.Precision.HIGHEST
    plane_xy = kernel_factors[0][:, :, None] * kernel_factors[1][:, None, :]
    kernel = jnp.einsum("gxy,gz->xyz", plane_xy, kernel_factors[2], precision=highest)

    def solve_one(replica):
        padded = jnp.pad(replica, ((0, M - N), (0, M - N), (0, M - N)))
        spectrum = jnp.fft.fftn(padded)
        potential_field = jnp.fft.ifftn(spectrum * kernel).real
        return potential_field[:N, :N, :N].astype(jnp.float32)

    return lax.map(solve_one, density)
```

```python
import math

import jax
import jax.numpy as jnp
import numpy as np
from jax import lax
from jax.sharding import PartitionSpec as P

HIGH = lax.Precision.HIGH


def spectral_table(length, chunks):
    freq = np.arange(length).reshape(chunks, 1, length // chunks, 1)
    angle = (freq * np.arange(length) % (2 * length)) * (math.pi / length)
    both = np.concatenate([np.cos(angle), np.sin(angle)], 1)
    return both.reshape(2 * length, length).astype(np.float32)


def dot(spec, left, right):
    return jnp.einsum(spec, left, right, precision=HIGH, preferred_element_type=jnp.float32)


def kernel_block(factors, y_start, y_count, z_start, z_count):
    length = factors.shape[2] // 2
    weights = np.full((length,), 1.0 / length, np.float32)
    weights[0] = 0.5 / length
    factors = factors[:, :, :length] * weights
    factor_y = lax.dynamic_slice_in_dim(factors[1], y_start, y_count, 1)
    factor_z = lax.dynamic_slice_in_dim(factors[2], z_start, z_count, 1)
    pair = factor_z[:, :, None] * factor_y[:, None, :]
    return jnp.einsum("gzy,gx->zyx", pair, factors[0], precision=lax.Precision.HIGHEST)


def body(density, kernel_factors):
    replicas, rows_x, rows_y, length = density.shape
    count_px = lax.axis_size("px")
    count_py = lax.axis_size("py")
    half = count_px // replicas
    trade = [[i + half * r for r in range(replicas)] for i in range(half)]
    lines = [[r * half + i for i in range(half)] for r in range(replicas)]
    index_x = lax.axis_index("px") % half
    index_y = lax.axis_index("py")
    table_z = spectral_table(length, count_py)
    table_y = spectral_table(length, half)
    order = np.arange(length).reshape(replicas, half, rows_x).transpose(1, 0, 2).reshape(-1)
    table_x = spectral_table(length, 1)[:, order]

    held = lax.all_to_all(density, "px", 0, 0, axis_index_groups=trade, tiled=True)
    held = held.reshape(replicas * rows_x, rows_y, length)
    held = dot("kz,xyz->kyx", table_z, held)
    held = lax.all_to_all(held, "py", 0, 1, tiled=True)
    held = dot("qy,kyx->kqx", table_y, held)
    held = lax.all_to_all(held, "px", 1, 2, axis_index_groups=lines, tiled=True)
    z_freq, y_freq = length // count_py, length // half
    kernel = kernel_block(kernel_factors, index_x * y_freq, y_freq, index_y * z_freq, z_freq)
    held = dot("kqx,px->kqp", held, table_x)
    held = held.reshape(2, z_freq, 2, y_freq, 2, length) * kernel[None, :, None, :, None, :]
    held = held.reshape(2 * z_freq, 2 * y_freq, 2 * length)
    held = dot("kqp,px->kqx", held, table_x)
    held = lax.all_to_all(held, "px", 2, 1, axis_index_groups=lines, tiled=True)
    held = dot("kqx,qy->kyx", held, table_y)
    held = lax.all_to_all(held, "py", 1, 0, tiled=True)
    held = dot("kyx,kz->xyz", held, table_z)
    held = held.reshape(replicas, rows_x, rows_y, length)
    return lax.all_to_all(held, "px", 0, 0, axis_index_groups=trade, tiled=True)


def solution(mesh):
    placed = (P("rep", "px", "py", None), P())
    return jax.shard_map(
        body, mesh=mesh, in_specs=placed, out_specs=P("rep", "px", "py", None), check_vma=False
    )
```

```python
import math

import jax
import jax.numpy as jnp
import numpy as np
from jax import lax
from jax.experimental import pallas as pl
from jax.experimental.pallas import tpu as pltpu
from jax.sharding import PartitionSpec as P

HIGHEST = lax.Precision.HIGHEST
BLOCK = 8


def spectral_table(length, chunks):
    freq = np.arange(length).reshape(chunks, 1, length // chunks, 1)
    angle = (freq * np.arange(length) % (2 * length)) * (math.pi / length)
    both = np.concatenate([np.cos(angle), np.sin(angle)], 1)
    return both.reshape(2 * length, length).astype(np.float32)


def dot(spec, left, right):
    return jnp.einsum(spec, left, right, precision=HIGHEST, preferred_element_type=jnp.float32)


def kernel_block(factors, y_start, y_count, z_start, z_count):
    length = factors.shape[2] // 2
    weights = np.full((length,), 1.0 / length, np.float32)
    weights[0] = 0.5 / length
    factors = factors[:, :, :length] * weights
    factor_y = lax.dynamic_slice_in_dim(factors[1], y_start, y_count, 1)
    factor_z = lax.dynamic_slice_in_dim(factors[2], z_start, z_count, 1)
    pair = factor_z[:, :, None] * factor_y[:, None, :]
    return jnp.einsum("gzy,gx->zyx", pair, factors[0], precision=lax.Precision.HIGHEST)


def plain_body(density, kernel_factors):
    replicas, rows_x, rows_y, length = density.shape
    count_px = lax.axis_size("px")
    count_py = lax.axis_size("py")
    half = count_px // replicas
    trade = [[i + half * r for r in range(replicas)] for i in range(half)]
    lines = [[r * half + i for i in range(half)] for r in range(replicas)]
    index_x = lax.axis_index("px") % half
    index_y = lax.axis_index("py")
    table_z = spectral_table(length, count_py)
    table_y = spectral_table(length, half)
    order = np.arange(length).reshape(replicas, half, rows_x).transpose(1, 0, 2).reshape(-1)
    table_x = spectral_table(length, 1)[:, order]

    held = lax.all_to_all(density, "px", 0, 0, axis_index_groups=trade, tiled=True)
    held = held.reshape(replicas * rows_x, rows_y, length)
    held = dot("kz,xyz->kyx", table_z, held)
    held = lax.all_to_all(held, "py", 0, 1, tiled=True)
    held = dot("qy,kyx->kqx", table_y, held)
    held = lax.all_to_all(held, "px", 1, 2, axis_index_groups=lines, tiled=True)
    z_freq, y_freq = length // count_py, length // half
    kernel = kernel_block(kernel_factors, index_x * y_freq, y_freq, index_y * z_freq, z_freq)
    held = dot("kqx,px->kqp", held, table_x)
    held = held.reshape(2, z_freq, 2, y_freq, 2, length) * kernel[None, :, None, :, None, :]
    held = held.reshape(2 * z_freq, 2 * y_freq, 2 * length)
    held = dot("kqp,px->kqx", held, table_x)
    held = lax.all_to_all(held, "px", 2, 1, axis_index_groups=lines, tiled=True)
    held = dot("kqx,qy->kyx", held, table_y)
    held = lax.all_to_all(held, "py", 1, 0, tiled=True)
    held = dot("kyx,kz->xyz", held, table_z)
    held = held.reshape(replicas, rows_x, rows_y, length)
    return lax.all_to_all(held, "px", 0, 0, axis_index_groups=trade, tiled=True)


def split(values, axis, third_low=False):
    high = values.astype(jnp.bfloat16)
    low = (values - high.astype(jnp.float32)).astype(jnp.bfloat16)
    return jnp.concatenate([high, high, low] if third_low else [high, low, high], axis)


def matmul(left, right, contract=((1,), (0,))):
    return lax.dot_general(left, right, (contract, ((), ())), preferred_element_type=jnp.float32)


def solve_kernel(
    dens, factors, fwd_z, fwd_y, fwd_x, inv_x, inv_y, inv_z, out,
    traded, a_send, a_held, b_send, b_held, g_send, g_held, h_send, h_held, o_send, o_held,
    sems_t, sems_z, sems_x, sems_xi, sems_zi, sems_ti,
):
    replicas, rows_x, rows_y, length = dens.shape
    count_py = lax.axis_size("py")
    half = lax.axis_size("px") // replicas
    me_px, me_py = lax.axis_index("px"), lax.axis_index("py")
    mine, line = lax.div(me_px, half), lax.rem(me_px, half)
    lanes = 2 * length // half
    mid = lanes // 2
    freq_z, freq_y = length // count_py, length // half
    blocks_y, blocks_f = rows_y // BLOCK, freq_z // BLOCK
    started = []

    def send(src, dst, sems, slot, device):
        copy = pltpu.make_async_remote_copy(
            src_ref=src, dst_ref=dst, send_sem=sems.at[(0,) + slot], recv_sem=sems.at[(1,) + slot],
            device_id=device, device_id_type=pl.DeviceIdType.MESH,
        )
        copy.start()
        started.append(copy)
        return copy

    trades = []
    for block in range(blocks_y):
        rows = pl.ds(block * BLOCK, BLOCK)
        for step in range(1, replicas):
            other = lax.rem(mine + step, replicas)
            trades.append(
                send(dens.at[other, :, rows, :], traded.at[mine, :, rows, :], sems_t,
                     (step, block), {"px": line + half * other})
            )
    traded[mine] = dens[mine]
    traded_rows = traded.reshape(replicas * rows_x * rows_y, length)
    a_rows = a_send.reshape(length * rows_y, lanes)

    arrivals = []
    for block in range(blocks_y):
        for copy in trades[block * (replicas - 1) : (block + 1) * (replicas - 1)]:
            copy.wait_recv()

        @pl.loop(0, BLOCK)
        def _(step, block=block):
            y = block * BLOCK + step
            cells = traded_rows[pl.ds(y, replicas * rows_x, stride=rows_y), :]
            waves = matmul(fwd_z[...], split(cells, 1), ((1,), (1,)))
            both = jnp.concatenate([waves[:length], waves[length:]], 1)
            a_rows[pl.ds(y, length, stride=rows_y), :] = both

        rows = pl.ds(block * BLOCK, BLOCK)
        there = pl.ds(pl.multiple_of(me_py * rows_y + block * BLOCK, BLOCK), BLOCK)
        for step in (2, 1, 3) if count_py == 4 else range(1, count_py):
            other = lax.rem(me_py + step, count_py)
            arrivals.append(
                send(a_send.at[pl.ds(other * freq_z, freq_z), rows, :], a_held.at[:, there, :],
                     sems_z, (step, block), {"py": other})
            )
        a_held[:, there, :] = a_send[pl.ds(me_py * freq_z, freq_z), rows, :]
    for copy in arrivals:
        copy.wait_recv()

    arrivals = []
    for block in range(blocks_f):

        @pl.loop(block * BLOCK, (block + 1) * BLOCK)
        def _(f):
            waves = matmul(fwd_y[...], split(a_held[f], 0))
            for part in range(half):
                b_send[part, f] = waves[part * 2 * freq_y : (part + 1) * 2 * freq_y]
            b_held[line, f] = b_send[line, f]

        some = pl.ds(block * BLOCK, BLOCK)
        here = []
        for step in range(1, half):
            other = lax.rem(line + step, half)
            here.append(
                send(b_send.at[other, some], b_held.at[line, some], sems_x, (step, block),
                     {"px": mine * half + other})
            )
        arrivals.append(here)

    factor_y = factors[1, pl.ds(pl.multiple_of(line * freq_y, BLOCK), freq_y), :]
    returns, arrivals_z = [], []

    def finish_lines(block):
        for copy in returns[block]:
            copy.wait_recv()

        @pl.loop(block * BLOCK, (block + 1) * BLOCK)
        def _(f):
            waves = jnp.concatenate([g_held[part, f] for part in range(half)], 0)
            h_send[f] = matmul(inv_y[...], split(waves, 0))
            own = pl.ds(pl.multiple_of(me_py * rows_y, BLOCK), rows_y)
            h_held[me_py * freq_z + f] = h_send[f, own, :]

        some = pl.ds(block * BLOCK, BLOCK)
        there = pl.ds(me_py * freq_z + block * BLOCK, BLOCK)
        for step in (2, 1, 3) if count_py == 4 else range(1, count_py):
            other = lax.rem(me_py + step, count_py)
            cells = pl.ds(pl.multiple_of(other * rows_y, BLOCK), rows_y)
            arrivals_z.append(
                send(h_send.at[some, cells, :], h_held.at[there], sems_zi, (step, block),
                     {"py": other})
            )

    for block in range(blocks_f):
        for copy in arrivals[block]:
            copy.wait_recv()

        @pl.loop(block * BLOCK, (block + 1) * BLOCK)
        def _(f):
            row = factors[2, pl.ds(me_py * freq_z + f, 1), :]
            kernel = lax.dot_general(
                factor_y * row, factors[0], (((1,), (1,)), ((), ())),
                precision=HIGHEST, preferred_element_type=jnp.float32,
            )
            kernel = jnp.concatenate([kernel, kernel], 1)
            kernel = jnp.concatenate([kernel] * 4, 0)
            ours = [b_held[part, f] for part in range(half)]
            cosines = jnp.concatenate([value[:, :mid] for value in ours], 1)
            sines = jnp.concatenate([value[:, mid:] for value in ours], 1)
            cells = jnp.concatenate([cosines, sines], 0)
            product = matmul(split(cells, 1), fwd_x[...]) * kernel
            cells = matmul(split(product, 1), inv_x[...])
            cosines, sines = cells[: 2 * freq_y], cells[2 * freq_y :]
            for part in range(half):
                cut = slice(part * mid, (part + 1) * mid)
                g_send[part, f] = jnp.concatenate([cosines[:, cut], sines[:, cut]], 1)
            g_held[line, f] = g_send[line, f]

        some = pl.ds(block * BLOCK, BLOCK)
        here = []
        for step in range(1, half):
            other = lax.rem(line + step, half)
            here.append(
                send(g_send.at[other, some], g_held.at[line, some], sems_xi, (step, block),
                     {"px": mine * half + other})
            )
        returns.append(here)
        if block:
            finish_lines(block - 1)
    finish_lines(blocks_f - 1)
    for copy in arrivals_z:
        copy.wait_recv()

    h_rows = h_held.reshape(length * rows_y, lanes)
    o_rows = o_send.reshape(replicas * rows_x * rows_y, length)
    arrivals = []
    for block in range(blocks_y):

        @pl.loop(block * BLOCK, (block + 1) * BLOCK)
        def _(y):
            waves = h_rows[pl.ds(y, length, stride=rows_y), :].T
            waves = jnp.concatenate([waves[:mid], waves[mid:]], 1)
            cells = matmul(split(waves, 1), inv_z[...])
            o_rows[pl.ds(y, replicas * rows_x, stride=rows_y), :] = cells

        rows = pl.ds(block * BLOCK, BLOCK)
        for step in range(1, replicas):
            other = lax.rem(mine + step, replicas)
            arrivals.append(
                send(o_send.at[other, :, rows, :], o_held.at[mine, :, rows, :], sems_ti,
                     (step, block), {"px": line + half * other})
            )
    out[mine] = o_send[mine]
    for copy in arrivals:
        copy.wait_recv()
    for step in range(1, replicas):
        other = lax.rem(mine + step, replicas)
        out[other] = o_held[other]
    for copy in started:
        copy.wait_send()


def kernel_body(density, kernel_factors):
    replicas, rows_x, rows_y, length = density.shape
    count_py = lax.axis_size("py")
    half = lax.axis_size("px") // replicas
    lanes = 2 * length // half
    freq_z, freq_y = length // count_py, length // half
    weights = np.full((length,), 1.0 / length, np.float32)
    weights[0] = 0.5 / length
    terms = kernel_factors.shape[1]
    factors = (kernel_factors[:, :, :length] * weights).transpose(0, 2, 1)
    factors = jnp.pad(factors, ((0, 0), (0, 0), (0, -terms % 128)))
    order = np.arange(length).reshape(replicas, half, rows_x).transpose(1, 0, 2).reshape(-1)
    table_z = spectral_table(length, 1)
    table_y = spectral_table(length, half)
    table_x = spectral_table(length, 1)[:, order]

    def held(table, axis):
        high = table.astype(jnp.bfloat16)
        low = (table - high.astype(np.float32)).astype(jnp.bfloat16)
        return jnp.asarray(np.concatenate([high, high, low], axis))

    tables = (
        held(table_z, 1), held(table_y, 1), held(table_x.T, 0),
        held(table_x, 0), held(table_y.T, 1), held(table_z, 0),
    )
    f32 = jnp.float32
    lines = (length, rows_y, lanes)
    whole = (freq_z, length, lanes)
    pairs = (half, freq_z, 2 * freq_y, lanes)
    blocks_y, blocks_f = rows_y // BLOCK, freq_z // BLOCK
    dma = pltpu.SemaphoreType.DMA
    return pl.pallas_call(
        solve_kernel,
        out_shape=jax.ShapeDtypeStruct(density.shape, f32),
        in_specs=[pl.BlockSpec(memory_space=pltpu.VMEM)] * 8,
        out_specs=pl.BlockSpec(memory_space=pltpu.VMEM),
        scratch_shapes=[
            pltpu.VMEM(density.shape, f32),
            pltpu.VMEM(lines, f32), pltpu.VMEM(whole, f32),
            pltpu.VMEM(pairs, f32), pltpu.VMEM(pairs, f32),
            pltpu.VMEM(pairs, f32), pltpu.VMEM(pairs, f32),
            pltpu.VMEM(whole, f32), pltpu.VMEM(lines, f32),
            pltpu.VMEM(density.shape, f32), pltpu.VMEM(density.shape, f32),
            dma((2, replicas, blocks_y)), dma((2, count_py, blocks_y)),
            dma((2, half, blocks_f)), dma((2, half, blocks_f)),
            dma((2, count_py, blocks_f)), dma((2, replicas, blocks_y)),
        ],
        compiler_params=pltpu.CompilerParams(
            has_side_effects=True, vmem_limit_bytes=56 * 2**20
        ),
    )(density, factors, *tables)


def body(density, kernel_factors):
    replicas, _, rows_y, length = density.shape
    lanes = 2 * length * replicas // lax.axis_size("px")
    freq_z = length // lax.axis_size("py")
    if lanes % 128 == 0 and rows_y % BLOCK == 0 and freq_z % BLOCK == 0:
        return kernel_body(density, kernel_factors)
    return plain_body(density, kernel_factors)


def solution(mesh):
    placed = (P("rep", "px", "py", None), P())
    return jax.shard_map(
        body, mesh=mesh, in_specs=placed, out_specs=P("rep", "px", "py", None), check_vma=False
    )
```

```python
import math

import jax
import jax.numpy as jnp
import numpy as np
from jax import lax
from jax.experimental import pallas as pl
from jax.experimental.pallas import tpu as pltpu
from jax.sharding import PartitionSpec as P

HIGHEST = lax.Precision.HIGHEST
BLOCK = 8


def spectral_table(length, chunks):
    freq = np.arange(length).reshape(chunks, 1, length // chunks, 1)
    angle = (freq * np.arange(length) % (2 * length)) * (math.pi / length)
    both = np.concatenate([np.cos(angle), np.sin(angle)], 1)
    return both.reshape(2 * length, length).astype(np.float32)


def dot(spec, left, right):
    return jnp.einsum(spec, left, right, precision=HIGHEST, preferred_element_type=jnp.float32)


def kernel_block(factors, y_start, y_count, z_start, z_count):
    length = factors.shape[2] // 2
    weights = np.full((length,), 1.0 / length, np.float32)
    weights[0] = 0.5 / length
    factors = factors[:, :, :length] * weights
    factor_y = lax.dynamic_slice_in_dim(factors[1], y_start, y_count, 1)
    factor_z = lax.dynamic_slice_in_dim(factors[2], z_start, z_count, 1)
    pair = factor_z[:, :, None] * factor_y[:, None, :]
    return jnp.einsum("gzy,gx->zyx", pair, factors[0], precision=lax.Precision.HIGHEST)


def plain_body(density, kernel_factors):
    replicas, rows_x, rows_y, length = density.shape
    count_px = lax.axis_size("px")
    count_py = lax.axis_size("py")
    half = count_px // replicas
    trade = [[i + half * r for r in range(replicas)] for i in range(half)]
    lines = [[r * half + i for i in range(half)] for r in range(replicas)]
    index_x = lax.axis_index("px") % half
    index_y = lax.axis_index("py")
    table_z = spectral_table(length, count_py)
    table_y = spectral_table(length, half)
    order = np.arange(length).reshape(replicas, half, rows_x).transpose(1, 0, 2).reshape(-1)
    table_x = spectral_table(length, 1)[:, order]

    held = lax.all_to_all(density, "px", 0, 0, axis_index_groups=trade, tiled=True)
    held = held.reshape(replicas * rows_x, rows_y, length)
    held = dot("kz,xyz->kyx", table_z, held)
    held = lax.all_to_all(held, "py", 0, 1, tiled=True)
    held = dot("qy,kyx->kqx", table_y, held)
    held = lax.all_to_all(held, "px", 1, 2, axis_index_groups=lines, tiled=True)
    z_freq, y_freq = length // count_py, length // half
    kernel = kernel_block(kernel_factors, index_x * y_freq, y_freq, index_y * z_freq, z_freq)
    held = dot("kqx,px->kqp", held, table_x)
    held = held.reshape(2, z_freq, 2, y_freq, 2, length) * kernel[None, :, None, :, None, :]
    held = held.reshape(2 * z_freq, 2 * y_freq, 2 * length)
    held = dot("kqp,px->kqx", held, table_x)
    held = lax.all_to_all(held, "px", 2, 1, axis_index_groups=lines, tiled=True)
    held = dot("kqx,qy->kyx", held, table_y)
    held = lax.all_to_all(held, "py", 1, 0, tiled=True)
    held = dot("kyx,kz->xyz", held, table_z)
    held = held.reshape(replicas, rows_x, rows_y, length)
    return lax.all_to_all(held, "px", 0, 0, axis_index_groups=trade, tiled=True)


def split(values, axis, third_low=False):
    high = values.astype(jnp.bfloat16)
    low = (values - high.astype(jnp.float32)).astype(jnp.bfloat16)
    return jnp.concatenate([high, high, low] if third_low else [high, low, high], axis)


def matmul(left, right, contract=((1,), (0,))):
    return lax.dot_general(left, right, (contract, ((), ())), preferred_element_type=jnp.float32)


def solve_kernel(
    dens, factors, fwd_z, fwd_y, fwd_x, inv_x, inv_y, inv_z, out,
    traded, a_send, a_held, b_send, b_held, g_send, g_held, h_send, h_held, o_send, o_held,
    sems_t, sems_z, sems_x, sems_xi, sems_zi, sems_ti,
):
    replicas, rows_x, rows_y, length = dens.shape
    count_py = lax.axis_size("py")
    half = lax.axis_size("px") // replicas
    me_px, me_py = lax.axis_index("px"), lax.axis_index("py")
    mine, line = lax.div(me_px, half), lax.rem(me_px, half)
    lanes = 2 * length // half
    mid = lanes // 2
    freq_z, freq_y = length // count_py, length // half
    blocks_y, blocks_f = rows_y // BLOCK, freq_z // BLOCK
    started = []

    def send(src, dst, sems, slot, device):
        copy = pltpu.make_async_remote_copy(
            src_ref=src, dst_ref=dst, send_sem=sems.at[(0,) + slot], recv_sem=sems.at[(1,) + slot],
            device_id=device, device_id_type=pl.DeviceIdType.MESH,
        )
        copy.start()
        started.append(copy)
        return copy

    trades = []
    for block in range(blocks_y):
        rows = pl.ds(block * BLOCK, BLOCK)
        for step in range(1, replicas):
            other = lax.rem(mine + step, replicas)
            trades.append(
                send(dens.at[other, :, rows, :], traded.at[mine, :, rows, :], sems_t,
                     (step, block), {"px": line + half * other})
            )
    traded[mine] = dens[mine]
    traded_rows = traded.reshape(replicas * rows_x * rows_y, length)
    a_rows = a_send.reshape(length * rows_y, lanes)

    first = blocks_y // 2
    peers = (2, 1, 3) if count_py == 4 else range(1, count_py)
    arrivals_y = [[] for _ in range(blocks_f)]

    def send_planes(freq, rows, there, slot):
        for step in peers:
            other = lax.rem(me_py + step, count_py)
            theirs = pl.ds(other * freq_z + freq.start, freq.size)
            arrivals_y[freq.start // BLOCK].append(
                send(a_send.at[theirs, rows, :], a_held.at[freq, there, :], sems_z,
                     (step, slot), {"py": other})
            )
        ours = pl.ds(me_py * freq_z + freq.start, freq.size)
        a_held[freq, there, :] = a_send[ours, rows, :]

    for block in range(blocks_y):
        for copy in trades[block * (replicas - 1) : (block + 1) * (replicas - 1)]:
            copy.wait_recv()

        @pl.loop(0, BLOCK)
        def _(step, block=block):
            y = block * BLOCK + step
            cells = traded_rows[pl.ds(y, replicas * rows_x, stride=rows_y), :]
            waves = matmul(fwd_z[...], split(cells, 1), ((1,), (1,)))
            both = jnp.concatenate([waves[:length], waves[length:]], 1)
            a_rows[pl.ds(y, length, stride=rows_y), :] = both

        if block < first:
            rows = pl.ds(block * BLOCK, BLOCK)
            there = pl.ds(pl.multiple_of(me_py * rows_y + block * BLOCK, BLOCK), BLOCK)
            send_planes(pl.ds(0, freq_z), rows, there, block)
    count = rows_y - first * BLOCK
    for block in range(blocks_f):
        rows = pl.ds(first * BLOCK, count)
        there = pl.ds(pl.multiple_of(me_py * rows_y + first * BLOCK, BLOCK), count)
        send_planes(pl.ds(block * BLOCK, BLOCK), rows, there, first + block)

    arrivals = []

    def start_lines(block):
        for copy in arrivals_y[block]:
            copy.wait_recv()

        @pl.loop(block * BLOCK, (block + 1) * BLOCK)
        def _(f):
            waves = matmul(fwd_y[...], split(a_held[f], 0))
            for part in range(half):
                b_send[part, f] = waves[part * 2 * freq_y : (part + 1) * 2 * freq_y]
            b_held[line, f] = b_send[line, f]

        some = pl.ds(block * BLOCK, BLOCK)
        here = []
        for step in range(1, half):
            other = lax.rem(line + step, half)
            here.append(
                send(b_send.at[other, some], b_held.at[line, some], sems_x, (step, block),
                     {"px": mine * half + other})
            )
        arrivals.append(here)

    factor_y = factors[1, pl.ds(pl.multiple_of(line * freq_y, BLOCK), freq_y), :]
    returns = []
    arrivals_z = [[] for _ in range(blocks_y)]

    def finish_lines(block):
        for copy in returns[block]:
            copy.wait_recv()

        @pl.loop(block * BLOCK, (block + 1) * BLOCK)
        def _(f):
            waves = jnp.concatenate([g_held[part, f] for part in range(half)], 0)
            h_send[f] = matmul(inv_y[...], split(waves, 0))
            own = pl.ds(pl.multiple_of(me_py * rows_y, BLOCK), rows_y)
            h_held[me_py * freq_z + f] = h_send[f, own, :]

        some = pl.ds(block * BLOCK, BLOCK)
        there = pl.ds(me_py * freq_z + block * BLOCK, BLOCK)
        last = block == blocks_f - 1
        size = BLOCK if last else rows_y
        for cut in range(rows_y // size):
            for step in peers:
                other = lax.rem(me_py + step, count_py)
                cells = pl.ds(pl.multiple_of(other * rows_y + cut * size, BLOCK), size)
                copy = send(
                    h_send.at[some, cells, :], h_held.at[there, pl.ds(cut * size, size), :],
                    sems_zi, (step, block + cut), {"py": other},
                )
                arrivals_z[cut].append(copy)

    def solve_lines(block):
        for copy in arrivals[block]:
            copy.wait_recv()

        @pl.loop(block * BLOCK, (block + 1) * BLOCK)
        def _(f):
            row = factors[2, pl.ds(me_py * freq_z + f, 1), :]
            kernel = lax.dot_general(
                factor_y * row, factors[0], (((1,), (1,)), ((), ())),
                precision=HIGHEST, preferred_element_type=jnp.float32,
            )
            kernel = jnp.concatenate([kernel, kernel], 1)
            kernel = jnp.concatenate([kernel] * 4, 0)
            ours = [b_held[part, f] for part in range(half)]
            cosines = jnp.concatenate([value[:, :mid] for value in ours], 1)
            sines = jnp.concatenate([value[:, mid:] for value in ours], 1)
            cells = jnp.concatenate([cosines, sines], 0)
            product = matmul(split(cells, 1), fwd_x[...]) * kernel
            cells = matmul(split(product, 1), inv_x[...])
            cosines, sines = cells[: 2 * freq_y], cells[2 * freq_y :]
            for part in range(half):
                cut = slice(part * mid, (part + 1) * mid)
                g_send[part, f] = jnp.concatenate([cosines[:, cut], sines[:, cut]], 1)
            g_held[line, f] = g_send[line, f]

        some = pl.ds(block * BLOCK, BLOCK)
        here = []
        for step in range(1, half):
            other = lax.rem(line + step, half)
            here.append(
                send(g_send.at[other, some], g_held.at[line, some], sems_xi, (step, block),
                     {"px": mine * half + other})
            )
        returns.append(here)

    for stage in range(blocks_f + 2):
        if stage < blocks_f:
            start_lines(stage)
        if 0 <= stage - 1 < blocks_f:
            solve_lines(stage - 1)
        if 0 <= stage - 2:
            finish_lines(stage - 2)

    h_rows = h_held.reshape(length * rows_y, lanes)
    o_rows = o_send.reshape(replicas * rows_x * rows_y, length)
    arrivals = []
    for block in range(blocks_y):
        for copy in arrivals_z[block]:
            copy.wait_recv()

        @pl.loop(block * BLOCK, (block + 1) * BLOCK)
        def _(y):
            waves = h_rows[pl.ds(y, length, stride=rows_y), :].T
            waves = jnp.concatenate([waves[:mid], waves[mid:]], 1)
            cells = matmul(split(waves, 1), inv_z[...])
            o_rows[pl.ds(y, replicas * rows_x, stride=rows_y), :] = cells

        rows = pl.ds(block * BLOCK, BLOCK)
        for step in range(1, replicas):
            other = lax.rem(mine + step, replicas)
            arrivals.append(
                send(o_send.at[other, :, rows, :], o_held.at[mine, :, rows, :], sems_ti,
                     (step, block), {"px": line + half * other})
            )
    out[mine] = o_send[mine]
    for copy in arrivals:
        copy.wait_recv()
    for step in range(1, replicas):
        other = lax.rem(mine + step, replicas)
        out[other] = o_held[other]
    for copy in started:
        copy.wait_send()


def kernel_body(density, kernel_factors):
    replicas, rows_x, rows_y, length = density.shape
    count_py = lax.axis_size("py")
    half = lax.axis_size("px") // replicas
    lanes = 2 * length // half
    freq_z, freq_y = length // count_py, length // half
    weights = np.full((length,), 1.0 / length, np.float32)
    weights[0] = 0.5 / length
    terms = kernel_factors.shape[1]
    factors = (kernel_factors[:, :, :length] * weights).transpose(0, 2, 1)
    factors = jnp.pad(factors, ((0, 0), (0, 0), (0, -terms % 128)))
    order = np.arange(length).reshape(replicas, half, rows_x).transpose(1, 0, 2).reshape(-1)
    table_z = spectral_table(length, 1)
    table_y = spectral_table(length, half)
    table_x = spectral_table(length, 1)[:, order]

    def held(table, axis):
        high = table.astype(jnp.bfloat16)
        low = (table - high.astype(np.float32)).astype(jnp.bfloat16)
        return jnp.asarray(np.concatenate([high, high, low], axis))

    tables = (
        held(table_z, 1), held(table_y, 1), held(table_x.T, 0),
        held(table_x, 0), held(table_y.T, 1), held(table_z, 0),
    )
    f32 = jnp.float32
    lines = (length, rows_y, lanes)
    whole = (freq_z, length, lanes)
    pairs = (half, freq_z, 2 * freq_y, lanes)
    blocks_y, blocks_f = rows_y // BLOCK, freq_z // BLOCK
    dma = pltpu.SemaphoreType.DMA
    return pl.pallas_call(
        solve_kernel,
        out_shape=jax.ShapeDtypeStruct(density.shape, f32),
        in_specs=[pl.BlockSpec(memory_space=pltpu.VMEM)] * 8,
        out_specs=pl.BlockSpec(memory_space=pltpu.VMEM),
        scratch_shapes=[
            pltpu.VMEM(density.shape, f32),
            pltpu.VMEM(lines, f32), pltpu.VMEM(whole, f32),
            pltpu.VMEM(pairs, f32), pltpu.VMEM(pairs, f32),
            pltpu.VMEM(pairs, f32), pltpu.VMEM(pairs, f32),
            pltpu.VMEM(whole, f32), pltpu.VMEM(lines, f32),
            pltpu.VMEM(density.shape, f32), pltpu.VMEM(density.shape, f32),
            dma((2, replicas, blocks_y)), dma((2, count_py, blocks_y // 2 + blocks_f)),
            dma((2, half, blocks_f)), dma((2, half, blocks_f)),
            dma((2, count_py, blocks_f + blocks_y)), dma((2, replicas, blocks_y)),
        ],
        compiler_params=pltpu.CompilerParams(
            has_side_effects=True, vmem_limit_bytes=56 * 2**20
        ),
    )(density, factors, *tables)


def body(density, kernel_factors):
    replicas, _, rows_y, length = density.shape
    lanes = 2 * length * replicas // lax.axis_size("px")
    freq_z = length // lax.axis_size("py")
    if lanes % 128 == 0 and rows_y % BLOCK == 0 and freq_z % BLOCK == 0:
        return kernel_body(density, kernel_factors)
    return plain_body(density, kernel_factors)


def solution(mesh):
    placed = (P("rep", "px", "py", None), P())
    return jax.shard_map(
        body, mesh=mesh, in_specs=placed, out_specs=P("rep", "px", "py", None), check_vma=False
    )
```

```python
import math

import jax
import jax.numpy as jnp
import numpy as np
from jax import lax
from jax.experimental import pallas as pl
from jax.experimental.pallas import tpu as pltpu
from jax.sharding import PartitionSpec as P

HIGHEST = lax.Precision.HIGHEST
BLOCK = 8


def spectral_table(length, chunks):
    freq = np.arange(length).reshape(chunks, 1, length // chunks, 1)
    angle = (freq * np.arange(length) % (2 * length)) * (math.pi / length)
    both = np.concatenate([np.cos(angle), np.sin(angle)], 1)
    return both.reshape(2 * length, length).astype(np.float32)


def dot(spec, left, right):
    return jnp.einsum(spec, left, right, precision=HIGHEST, preferred_element_type=jnp.float32)


def kernel_block(factors, y_start, y_count, z_start, z_count):
    length = factors.shape[2] // 2
    weights = np.full((length,), 1.0 / length, np.float32)
    weights[0] = 0.5 / length
    factors = factors[:, :, :length] * weights
    factor_y = lax.dynamic_slice_in_dim(factors[1], y_start, y_count, 1)
    factor_z = lax.dynamic_slice_in_dim(factors[2], z_start, z_count, 1)
    pair = factor_z[:, :, None] * factor_y[:, None, :]
    return jnp.einsum("gzy,gx->zyx", pair, factors[0], precision=lax.Precision.HIGHEST)


def plain_body(density, kernel_factors):
    replicas, rows_x, rows_y, length = density.shape
    count_px = lax.axis_size("px")
    count_py = lax.axis_size("py")
    half = count_px // replicas
    trade = [[i + half * r for r in range(replicas)] for i in range(half)]
    lines = [[r * half + i for i in range(half)] for r in range(replicas)]
    index_x = lax.axis_index("px") % half
    index_y = lax.axis_index("py")
    table_z = spectral_table(length, count_py)
    table_y = spectral_table(length, half)
    order = np.arange(length).reshape(replicas, half, rows_x).transpose(1, 0, 2).reshape(-1)
    table_x = spectral_table(length, 1)[:, order]

    held = lax.all_to_all(density, "px", 0, 0, axis_index_groups=trade, tiled=True)
    held = held.reshape(replicas * rows_x, rows_y, length)
    held = dot("kz,xyz->kyx", table_z, held)
    held = lax.all_to_all(held, "py", 0, 1, tiled=True)
    held = dot("qy,kyx->kqx", table_y, held)
    held = lax.all_to_all(held, "px", 1, 2, axis_index_groups=lines, tiled=True)
    z_freq, y_freq = length // count_py, length // half
    kernel = kernel_block(kernel_factors, index_x * y_freq, y_freq, index_y * z_freq, z_freq)
    held = dot("kqx,px->kqp", held, table_x)
    held = held.reshape(2, z_freq, 2, y_freq, 2, length) * kernel[None, :, None, :, None, :]
    held = held.reshape(2 * z_freq, 2 * y_freq, 2 * length)
    held = dot("kqp,px->kqx", held, table_x)
    held = lax.all_to_all(held, "px", 2, 1, axis_index_groups=lines, tiled=True)
    held = dot("kqx,qy->kyx", held, table_y)
    held = lax.all_to_all(held, "py", 1, 0, tiled=True)
    held = dot("kyx,kz->xyz", held, table_z)
    held = held.reshape(replicas, rows_x, rows_y, length)
    return lax.all_to_all(held, "px", 0, 0, axis_index_groups=trade, tiled=True)


def split(values, axis, third_low=False):
    high = values.astype(jnp.bfloat16)
    low = (values - high.astype(jnp.float32)).astype(jnp.bfloat16)
    return jnp.concatenate([high, high, low] if third_low else [high, low, high], axis)


def matmul(left, right, contract=((1,), (0,))):
    return lax.dot_general(left, right, (contract, ((), ())), preferred_element_type=jnp.float32)


def solve_kernel(
    dens, factors, fwd_z, fwd_y, fwd_x, inv_x, inv_y, inv_z, out,
    traded, a_send, a_held, b_send, b_held, g_send, g_held, h_send, h_held, o_send, o_held,
    sems_t, sems_z, sems_x, sems_xi, sems_zi, sems_ti,
):
    replicas, rows_x, rows_y, length = dens.shape
    count_py = lax.axis_size("py")
    half = lax.axis_size("px") // replicas
    me_px, me_py = lax.axis_index("px"), lax.axis_index("py")
    mine, line = lax.div(me_px, half), lax.rem(me_px, half)
    lanes = 2 * length // half
    mid = lanes // 2
    freq_z, freq_y = length // count_py, length // half
    blocks_y, blocks_f = rows_y // BLOCK, freq_z // BLOCK
    started = []

    def send(src, dst, sems, slot, device):
        copy = pltpu.make_async_remote_copy(
            src_ref=src, dst_ref=dst, send_sem=sems.at[(0,) + slot], recv_sem=sems.at[(1,) + slot],
            device_id=device, device_id_type=pl.DeviceIdType.MESH,
        )
        copy.start()
        started.append(copy)
        return copy

    trades = []
    for block in range(blocks_y):
        rows = pl.ds(block * BLOCK, BLOCK)
        for step in range(1, replicas):
            other = lax.rem(mine + step, replicas)
            trades.append(
                send(dens.at[other, :, rows, :], traded.at[mine, :, rows, :], sems_t,
                     (step, block), {"px": line + half * other})
            )
    traded[mine] = dens[mine]
    traded_rows = traded.reshape(replicas * rows_x * rows_y, length)
    a_rows = a_send.reshape(length * rows_y, lanes)

    first = blocks_y // 4
    peers = (2, 1, 3) if count_py == 4 else range(1, count_py)
    arrivals_y = [[] for _ in range(blocks_f)]

    def send_planes(freq, rows, there, slot):
        for step in peers:
            other = lax.rem(me_py + step, count_py)
            theirs = pl.ds(other * freq_z + freq.start, freq.size)
            arrivals_y[freq.start // BLOCK].append(
                send(a_send.at[theirs, rows, :], a_held.at[freq, there, :], sems_z,
                     (step, slot), {"py": other})
            )
        ours = pl.ds(me_py * freq_z + freq.start, freq.size)
        a_held[freq, there, :] = a_send[ours, rows, :]

    for block in range(blocks_y):
        for copy in trades[block * (replicas - 1) : (block + 1) * (replicas - 1)]:
            copy.wait_recv()

        @pl.loop(0, BLOCK, unroll=4)
        def _(step, block=block):
            y = block * BLOCK + step
            cells = traded_rows[pl.ds(y, replicas * rows_x, stride=rows_y), :]
            waves = matmul(fwd_z[...], split(cells, 1), ((1,), (1,)))
            both = jnp.concatenate([waves[:length], waves[length:]], 1)
            a_rows[pl.ds(y, length, stride=rows_y), :] = both

        if block < first:
            rows = pl.ds(block * BLOCK, BLOCK)
            there = pl.ds(pl.multiple_of(me_py * rows_y + block * BLOCK, BLOCK), BLOCK)
            send_planes(pl.ds(0, freq_z), rows, there, block)
    count = rows_y - first * BLOCK
    for block in range(blocks_f):
        rows = pl.ds(first * BLOCK, count)
        there = pl.ds(pl.multiple_of(me_py * rows_y + first * BLOCK, BLOCK), count)
        send_planes(pl.ds(block * BLOCK, BLOCK), rows, there, first + block)

    arrivals = []

    def start_lines(block):
        for copy in arrivals_y[block]:
            copy.wait_recv()

        @pl.loop(block * BLOCK, (block + 1) * BLOCK, unroll=4)
        def _(f):
            waves = matmul(fwd_y[...], split(a_held[f], 0))
            for part in range(half):
                b_send[part, f] = waves[part * 2 * freq_y : (part + 1) * 2 * freq_y]
            b_held[line, f] = b_send[line, f]

        some = pl.ds(block * BLOCK, BLOCK)
        here = []
        for step in range(1, half):
            other = lax.rem(line + step, half)
            here.append(
                send(b_send.at[other, some], b_held.at[line, some], sems_x, (step, block),
                     {"px": mine * half + other})
            )
        arrivals.append(here)

    factor_y = factors[1, pl.ds(pl.multiple_of(line * freq_y, BLOCK), freq_y), :]
    returns = []
    arrivals_z = [[] for _ in range(blocks_y)]

    def finish_lines(block):
        for copy in returns[block]:
            copy.wait_recv()

        @pl.loop(block * BLOCK, (block + 1) * BLOCK, unroll=4)
        def _(f):
            waves = jnp.concatenate([g_held[part, f] for part in range(half)], 0)
            h_send[f] = matmul(inv_y[...], split(waves, 0))
            own = pl.ds(pl.multiple_of(me_py * rows_y, BLOCK), rows_y)
            h_held[me_py * freq_z + f] = h_send[f, own, :]

        some = pl.ds(block * BLOCK, BLOCK)
        there = pl.ds(me_py * freq_z + block * BLOCK, BLOCK)
        last = block == blocks_f - 1
        size = BLOCK if last else rows_y
        for cut in range(rows_y // size):
            for step in peers:
                other = lax.rem(me_py + step, count_py)
                cells = pl.ds(pl.multiple_of(other * rows_y + cut * size, BLOCK), size)
                copy = send(
                    h_send.at[some, cells, :], h_held.at[there, pl.ds(cut * size, size), :],
                    sems_zi, (step, block + cut), {"py": other},
                )
                arrivals_z[cut].append(copy)

    def solve_lines(block):
        for copy in arrivals[block]:
            copy.wait_recv()

        @pl.loop(block * BLOCK, (block + 1) * BLOCK, unroll=4)
        def _(f):
            row = factors[2, pl.ds(me_py * freq_z + f, 1), :]
            kernel = lax.dot_general(
                factor_y * row, factors[0], (((1,), (1,)), ((), ())),
                precision=HIGHEST, preferred_element_type=jnp.float32,
            )
            kernel = jnp.concatenate([kernel, kernel], 1)
            kernel = jnp.concatenate([kernel] * 4, 0)
            ours = [b_held[part, f] for part in range(half)]
            cosines = jnp.concatenate([value[:, :mid] for value in ours], 1)
            sines = jnp.concatenate([value[:, mid:] for value in ours], 1)
            cells = jnp.concatenate([cosines, sines], 0)
            product = matmul(split(cells, 1), fwd_x[...]) * kernel
            cells = matmul(split(product, 1), inv_x[...])
            cosines, sines = cells[: 2 * freq_y], cells[2 * freq_y :]
            for part in range(half):
                cut = slice(part * mid, (part + 1) * mid)
                g_send[part, f] = jnp.concatenate([cosines[:, cut], sines[:, cut]], 1)
            g_held[line, f] = g_send[line, f]

        some = pl.ds(block * BLOCK, BLOCK)
        here = []
        for step in range(1, half):
            other = lax.rem(line + step, half)
            here.append(
                send(g_send.at[other, some], g_held.at[line, some], sems_xi, (step, block),
                     {"px": mine * half + other})
            )
        returns.append(here)

    for stage in range(blocks_f + 2):
        if stage < blocks_f:
            start_lines(stage)
        if 0 <= stage - 1 < blocks_f:
            solve_lines(stage - 1)
        if 0 <= stage - 2:
            finish_lines(stage - 2)

    h_rows = h_held.reshape(length * rows_y, lanes)
    o_rows = o_send.reshape(replicas * rows_x * rows_y, length)
    arrivals = []
    for block in range(blocks_y):
        for copy in arrivals_z[block]:
            copy.wait_recv()

        @pl.loop(block * BLOCK, (block + 1) * BLOCK, unroll=4)
        def _(y):
            waves = h_rows[pl.ds(y, length, stride=rows_y), :].T
            waves = jnp.concatenate([waves[:mid], waves[mid:]], 1)
            cells = matmul(split(waves, 1), inv_z[...])
            o_rows[pl.ds(y, replicas * rows_x, stride=rows_y), :] = cells

        rows = pl.ds(block * BLOCK, BLOCK)
        for step in range(1, replicas):
            other = lax.rem(mine + step, replicas)
            arrivals.append(
                send(o_send.at[other, :, rows, :], o_held.at[mine, :, rows, :], sems_ti,
                     (step, block), {"px": line + half * other})
            )
    out[mine] = o_send[mine]
    for copy in arrivals:
        copy.wait_recv()
    for step in range(1, replicas):
        other = lax.rem(mine + step, replicas)
        out[other] = o_held[other]
    for copy in started:
        copy.wait_send()


def kernel_body(density, kernel_factors):
    replicas, rows_x, rows_y, length = density.shape
    count_py = lax.axis_size("py")
    half = lax.axis_size("px") // replicas
    lanes = 2 * length // half
    freq_z, freq_y = length // count_py, length // half
    weights = np.full((length,), 1.0 / length, np.float32)
    weights[0] = 0.5 / length
    terms = kernel_factors.shape[1]
    factors = (kernel_factors[:, :, :length] * weights).transpose(0, 2, 1)
    factors = jnp.pad(factors, ((0, 0), (0, 0), (0, -terms % 128)))
    order = np.arange(length).reshape(replicas, half, rows_x).transpose(1, 0, 2).reshape(-1)
    table_z = spectral_table(length, 1)
    table_y = spectral_table(length, half)
    table_x = spectral_table(length, 1)[:, order]

    def held(table, axis):
        high = table.astype(jnp.bfloat16)
        low = (table - high.astype(np.float32)).astype(jnp.bfloat16)
        return jnp.asarray(np.concatenate([high, high, low], axis))

    tables = (
        held(table_z, 1), held(table_y, 1), held(table_x.T, 0),
        held(table_x, 0), held(table_y.T, 1), held(table_z, 0),
    )
    f32 = jnp.float32
    lines = (length, rows_y, lanes)
    whole = (freq_z, length, lanes)
    pairs = (half, freq_z, 2 * freq_y, lanes)
    blocks_y, blocks_f = rows_y // BLOCK, freq_z // BLOCK
    dma = pltpu.SemaphoreType.DMA
    return pl.pallas_call(
        solve_kernel,
        out_shape=jax.ShapeDtypeStruct(density.shape, f32),
        in_specs=[pl.BlockSpec(memory_space=pltpu.VMEM)] * 8,
        out_specs=pl.BlockSpec(memory_space=pltpu.VMEM),
        scratch_shapes=[
            pltpu.VMEM(density.shape, f32),
            pltpu.VMEM(lines, f32), pltpu.VMEM(whole, f32),
            pltpu.VMEM(pairs, f32), pltpu.VMEM(pairs, f32),
            pltpu.VMEM(pairs, f32), pltpu.VMEM(pairs, f32),
            pltpu.VMEM(whole, f32), pltpu.VMEM(lines, f32),
            pltpu.VMEM(density.shape, f32), pltpu.VMEM(density.shape, f32),
            dma((2, replicas, blocks_y)), dma((2, count_py, blocks_y // 2 + blocks_f)),
            dma((2, half, blocks_f)), dma((2, half, blocks_f)),
            dma((2, count_py, blocks_f + blocks_y)), dma((2, replicas, blocks_y)),
        ],
        compiler_params=pltpu.CompilerParams(
            has_side_effects=True, vmem_limit_bytes=56 * 2**20
        ),
    )(density, factors, *tables)


def body(density, kernel_factors):
    replicas, _, rows_y, length = density.shape
    lanes = 2 * length * replicas // lax.axis_size("px")
    freq_z = length // lax.axis_size("py")
    if lanes % 128 == 0 and rows_y % BLOCK == 0 and freq_z % BLOCK == 0:
        return kernel_body(density, kernel_factors)
    return plain_body(density, kernel_factors)


def solution(mesh):
    placed = (P("rep", "px", "py", None), P())
    return jax.shard_map(
        body, mesh=mesh, in_specs=placed, out_specs=P("rep", "px", "py", None), check_vma=False
    )
```
